256 devices in a mesh: tile: 32 (over y, z), lat: 4 (over x), emu: 2 (over core).
Axes of the slice: x: 4, y: 4, z: 8, core: 2. Of those that a mesh axis runs over, the one named last changes fastest.
Arguments:
- state: float32 [512, 128, 12, 128], P('tile', ('lat', 'emu')), may hold values from -6 to 6
- diffusivity: float32 [12, 128], replicated, may hold values from 0.03 to 0.2
- wind: float32 [512, 128], P('tile', ('lat', 'emu')), may hold values from -0.5 to 0.5
- land_mask: int32 [512, 128], P('tile', ('lat', 'emu')), may hold values 0 or 1
- routes: int32 [32, 4, 2, 256, 1], P('tile', 'lat', 'emu'), may hold values from 0 to 127; in each aligned block of 256 rows (0 to 255, 256 to 511, ..., all dimensions but the last counted through in order) at most 2 rows name the same one
- counts: int32 [32, 4, 2], P('tile', 'lat', 'emu'), may hold values from 64 to 256
- w_in: bfloat16 [128, 1536, 1024], P(('tile', 'lat')), may hold values from -0.15625 to 0.15625
- b_in: float32 [128, 1024], P(('tile', 'lat')), may hold values from -3 to 3
- land_vec: float32 [128, 1024], P(('tile', 'lat')), may hold values from -5 to 5
- w_hid: bfloat16 [128, 2, 1024, 1024], P(('tile', 'lat')), may hold values from -0.1875 to 0.1875
- b_hid: float32 [128, 2, 1024], P(('tile', 'lat')), may hold values from -3 to 3
- w_out: bfloat16 [128, 1024, 512], P(('tile', 'lat')), may hold values from -0.1875 to 0.1875
Outputs:
- updated: float32 [512, 128, 4, 128], P('tile', ('lat', 'emu'))
The draws below stay inside these ranges and needn't reach their ends.
Inputs may be any that keep to these rules, and one draw needn't show every extreme that they name: `routes`: among the 256 columns of one device, at most 2 name the same expert.
All inputs are finite; a program needn't handle non-finite values. No bound on the sum of `land_mask` on one device may be relied on, other than what follows from the above.
Results may differ from the reference program's by a relative error of at most 0.0026.
Values may be sent and summed in bfloat16 or wider, within the bound.
A program may use at most 64 MiB of HBM per device.

```python
import math
import jax
import jax.numpy as jnp
import numpy as np
from jax import lax

LEV = 128
VARS = 12
HID = 1024
OUTV = 4
LAYERS = 2
CLON = 16
CLAT = 16
COLS_DEV = 256
EXPERTS = 128
CAP = 2
NLON = 512
NLAT = 128
N_TILE = 32
N_LAT = 4
N_EMU = 2


def set_ends(values, own_key, smallest, largest):
    spot = [jax.random.randint(jax.random.fold_in(own_key, axis), (), 0, length) for axis, length in enumerate(values.shape)]
    longest = values.shape.index(max(values.shape))
    neighbour = spot[:longest] + [(spot[longest] + 1) % values.shape[longest]] + spot[longest + 1:]
    return values.at[tuple(spot)].set(smallest).at[tuple(neighbour)].set(largest)


def shard_levels(stream_key, dims, pieces, low, largest):
    def one(dim, blocks):
        steps = jax.random.uniform(jax.random.fold_in(jax.random.fold_in(stream_key, 6), dim), (blocks,), jnp.float32, low / len(pieces), largest / len(pieces))
        return jnp.repeat(jnp.exp(steps), dims[dim] // blocks).reshape((-1,) + (1,) * (len(dims) - dim - 1))

    level = one(*pieces[0])
    for cut in pieces[1:]:
        level = level * one(*cut)
    return level


def deal_out(rng, own, number, rows, amount, top, most, skew):
    order = jax.random.permutation(rng, amount)
    heavy_load, usual = portions_of(amount, rows * top, most, skew, True), portions_of(amount, rows * top, most, skew, False)
    places = jnp.arange(amount)

    def named(tallies, rotation):
        used = int((tallies > 0).sum())
        fixed = max(1, used // 4)
        moved = fixed + (places - fixed + rotation * (used - fixed)) % max(1, amount - fixed)
        return jnp.zeros((amount,), jnp.int32).at[order[jnp.where(places < fixed, places, moved)]].set(jnp.asarray(tallies, jnp.int32))

    tallies = jnp.where(number % 4 == 0, named(heavy_load, number // 4), named(usual, number - number // 4 - 1))
    mixed = jax.random.permutation(jax.random.fold_in(own, 3), amount)
    source_of, sink = mixed[0:amount // 2 * 2:2], mixed[1:amount // 2 * 2:2]
    room = jnp.minimum(tallies[source_of] - 1, most - tallies[sink]) // 2
    room = jnp.where((source_of == order[0]) | (sink == order[0]) | (tallies[sink] == 0), 0, jnp.maximum(room, 0))
    moved = jax.random.randint(jax.random.fold_in(own, 4), (amount // 2,), 0, 1 << 20) % (room + 1)
    tallies = tallies.at[source_of].add(-moved).at[sink].add(moved)
    members = jnp.searchsorted(jnp.cumsum(tallies), jnp.arange(rows * top), side="right").astype(jnp.int32)
    listing = members.reshape(top, rows).T
    listing = listing[jax.random.permutation(jax.random.fold_in(own, 1), rows)]
    rotation = jax.random.randint(jax.random.fold_in(own, 2), (rows, 1), 0, top)
    return jnp.take_along_axis(listing, (jnp.arange(top)[None, :] + rotation) % top, axis=1)


def portions_of(count, total, reach, skew, full):
    weights = [(1 << 20) // math.isqrt(grade ** skew) + 1 for grade in range(1, count + 1)]
    largest = reach if full else min(reach, max(-(-total // count), total * weights[0] // sum(weights)))
    least = 1 if total - largest >= count - 1 else 0
    given, rest = [largest] + [least] * (count - 1), total - largest - least * (count - 1)
    while rest > 0:
        free = [i for i in range(1, count) if given[i] < largest] or [i for i in range(1, count) if given[i] < reach]
        whole, budget = sum([weights[i] for i in free]), rest
        for i in free:
            extra = min(reach - given[i], max(1, budget * weights[i] // whole), rest)
            given[i] = given[i] + extra
            rest = rest - extra
    return np.array(given)


def noise(own_key, shape, scale, most, split=(), held_as=jnp.bfloat16):
    result = jax.random.normal(own_key, shape, jnp.float32) * scale
    if len(split) > 0:
        result = shard_levels(own_key, shape, split, -0.22, 0.18) * result
    return jnp.clip(result, min=-most, max=most).astype(held_as)


def setup_inputs(seed: int = 0) -> dict:
    arg_keys = jax.random.split(jax.random.key(seed), 13)
    state = noise(arg_keys[0], (NLON, NLAT, VARS, LEV), 1.0, 6.0, ((0, 32), (1, 8)), jnp.float32)
    diffusivity = jnp.clip(jnp.exp(jax.random.uniform(arg_keys[1], (VARS, LEV), jnp.float32, math.log(0.03), math.log(0.2))), 0.03, 0.2)
    wind = jnp.clip(jax.random.uniform(arg_keys[2], (NLON, NLAT), jnp.float32, -0.5, 0.5) * shard_levels(arg_keys[2], (NLON, NLAT), ((0, 32), (1, 8)), -0.4, 0.0), -0.5, 0.5)
    land_mask = set_ends((jax.random.randint(arg_keys[3], (NLON, NLAT), 0, 3) < 1).astype(jnp.int32), jax.random.fold_in(arg_keys[3], 1), 0, 1)
    routes_keys = jax.random.split(jax.random.fold_in(arg_keys[4], 1), N_TILE * N_LAT * N_EMU * COLS_DEV // COLS_DEV)
    routes_turns = jax.random.permutation(jax.random.fold_in(arg_keys[4], 3), N_TILE * N_LAT * N_EMU * COLS_DEV // COLS_DEV)
    routes = jax.vmap(lambda own, number: deal_out(jax.random.fold_in(arg_keys[4], 2), own, number, COLS_DEV, EXPERTS, 1, CAP, 2))(routes_keys, routes_turns).reshape((N_TILE, N_LAT, N_EMU, COLS_DEV, 1))
    counts = set_ends(jax.random.randint(arg_keys[5], (N_TILE, N_LAT, N_EMU), COLS_DEV // 4, COLS_DEV + 1), jax.random.fold_in(arg_keys[5], 1), COLS_DEV // 4, COLS_DEV).astype(jnp.int32)
    w_in = noise(arg_keys[6], (EXPERTS, VARS * LEV, HID), (VARS * LEV) ** -0.5, 0.15625, ((0, 128),))
    b_in = noise(arg_keys[7], (EXPERTS, HID), 0.5, 3.0, ((0, 128),), jnp.float32)
    land_vec = noise(arg_keys[8], (EXPERTS, HID), 1.0, 5.0, ((0, 128),), jnp.float32)
    w_hid = noise(arg_keys[9], (EXPERTS, LAYERS, HID, HID), HID ** -0.5, 0.1875, ((0, 128),))
    b_hid = noise(arg_keys[10], (EXPERTS, LAYERS, HID), 0.5, 3.0, ((0, 128),), jnp.float32)
    w_out = noise(arg_keys[11], (EXPERTS, HID, OUTV * LEV), HID ** -0.5, 0.1875, ((0, 128),))
    return {"state": state, "diffusivity": diffusivity, "wind": wind, "land_mask": land_mask, "routes": routes, "counts": counts, "w_in": w_in, "b_in": b_in, "land_vec": land_vec, "w_hid": w_hid, "b_hid": b_hid, "w_out": w_out}


def advance(center, east, west, north, south, diffusivity, wind):
    spread = east + west + north + south - 4.0 * center
    return center + diffusivity[None, None] * spread - 0.5 * wind[:, :, None, None] * (east - west)


def column_slots(route_flat, count, experts, capacity):
    columns = route_flat.shape[0]
    positions = jnp.arange(columns, dtype=jnp.int32)
    active = positions < count
    onehot = ((route_flat[:, None] == jnp.arange(experts, dtype=jnp.int32)[None, :]) & active[:, None]).astype(jnp.int32)
    before = jnp.cumsum(onehot, axis=0) - onehot
    ranking = jnp.sum(before * onehot, axis=1).astype(jnp.int32)
    slot_index = jnp.where(active, route_flat * capacity + ranking, experts * capacity)
    return slot_index.astype(jnp.int32), active


def run_network(features, flags, w_first, b_first, land_add, w_inner, b_inner, w_last):
    lead = features.shape[:-1]
    rows = features.reshape(-1, features.shape[-1])
    pre = jnp.dot(rows, w_first, preferred_element_type=jnp.float32) + b_first[None, :]
    pre = pre + flags.reshape(-1, 1).astype(jnp.float32) * land_add[None, :]
    hidden = jax.nn.silu(pre).astype(jnp.bfloat16)
    for number in range(w_inner.shape[0]):
        inner = jnp.dot(hidden, w_inner[number], preferred_element_type=jnp.float32) + b_inner[number][None, :]
        hidden = jax.nn.silu(inner).astype(jnp.bfloat16)
    produced = jnp.dot(hidden, w_last, preferred_element_type=jnp.float32).astype(jnp.bfloat16)
    return produced.reshape(lead + (w_last.shape[1],))


def place_rows(slot_index, values, experts, capacity):
    width = values.shape[-1]
    filled = jnp.zeros((experts * capacity + 1, width), values.dtype).at[slot_index].set(values)
    return filled[:-1].reshape(experts, capacity, width)


def pick_rows(slot_index, returned):
    width = returned.shape[-1]
    flat = jnp.concatenate([returned.reshape(-1, width), jnp.zeros((1, width), returned.dtype)], axis=0)
    return flat[slot_index]


def reference(state, diffusivity, wind, land_mask, routes, counts, w_in, b_in, land_vec, w_hid, b_hid, w_out):
    east = jnp.roll(state, -1, axis=0)
    west = jnp.roll(state, 1, axis=0)
    padded = jnp.pad(state, ((0, 0), (1, 1), (0, 0), (0, 0)))
    advanced = advance(state, east, west, padded[:, 2:], padded[:, :-2], diffusivity, wind)
    experts = N_TILE * N_LAT
    fsize = VARS * LEV
    columns = CLON * CLAT
    features = advanced.astype(jnp.bfloat16).reshape(N_TILE, CLON, N_LAT, N_EMU, CLAT, fsize)
    features = features.transpose(0, 2, 3, 1, 4, 5).reshape(experts, N_EMU, columns, fsize)
    land = land_mask.reshape(N_TILE, CLON, N_LAT, N_EMU, CLAT).transpose(0, 2, 3, 1, 4)
    land = land.reshape(experts, N_EMU, columns, 1).astype(jnp.bfloat16)
    route_cols = routes.reshape(experts, N_EMU, columns).astype(jnp.int32)
    count_dev = counts.reshape(experts, N_EMU).astype(jnp.int32)

    def slot_of(route_flat, count):
        return column_slots(route_flat, count, experts, CAP)[0]

    slot_index = jax.vmap(jax.vmap(slot_of))(route_cols, count_dev)

    def place(slots, values):
        return place_rows(slots, values, experts, CAP)

    outbound = jax.vmap(jax.vmap(place))(slot_index, features)
    flags = jax.vmap(jax.vmap(place))(slot_index, land)

    def serve(items):
        return run_network(items[0], items[1], items[2], items[3], items[4], items[5], items[6], items[7])

    produced = lax.map(serve, (jnp.moveaxis(outbound, 2, 0), jnp.moveaxis(flags, 2, 0), w_in, b_in, land_vec, w_hid, b_hid, w_out))
    returned = jnp.moveaxis(produced, 0, 2)
    tendency = jax.vmap(jax.vmap(pick_rows))(slot_index, returned).astype(jnp.float32)
    tendency = tendency.reshape(N_TILE, N_LAT, N_EMU, CLON, CLAT, OUTV, LEV).transpose(0, 3, 1, 2, 4, 5, 6)
    tendency = tendency.reshape(NLON, NLAT, OUTV, LEV)
    return advanced[:, :, :OUTV, :] + tendency
```

```python
import functools

import jax
import jax.numpy as jnp
from jax import lax
from jax.experimental import pallas as pl
from jax.experimental.pallas import tpu as pltpu
from jax.sharding import PartitionSpec as P

MESH = pl.DeviceIdType.MESH
BF16 = jnp.bfloat16
F32 = jnp.float32

NY, NZ, NX = 4, 8, 4
PLANE = NY * NX
PEERS = PLANE * NZ
LON, LAT, VARS, LEV, OUTV = 16, 16, 12, 128, 4
COLS = LON * LAT
ROWS = VARS * LAT
HID = 1024
WORDS = VARS + 1


def place(step, z_off, me):
    y, z, lat = me
    d_x, d_y = lax.rem(step, NX), lax.div(step, NX)
    tile = lax.rem(y + d_y, NY) * NZ + lax.rem(z + z_off, NZ)
    return tile, lax.rem(lat + d_x, NX)


def source(step, z_off, me):
    y, z, lat = me
    d_x, d_y = lax.rem(step, NX), lax.div(step, NX)
    tile = lax.rem(y + NY - d_y, NY) * NZ + lax.rem(z + NZ - z_off, NZ)
    return tile, lax.rem(lat + NX - d_x, NX)


def slot_row(route_row, count):
    shape = (COLS, COLS)
    first = lax.broadcasted_iota(jnp.int32, shape, 0)
    second = lax.broadcasted_iota(jnp.int32, shape, 1)
    row = jnp.broadcast_to(route_row, shape)
    diagonal = jnp.where(first == second, row, 0.0)
    column = jnp.broadcast_to(jnp.sum(diagonal, axis=1, keepdims=True), shape)
    earlier = (first < second) & (row == column) & (first < count)
    rank = jnp.sum(jnp.where(earlier, 1.0, 0.0), axis=0, keepdims=True)
    position = lax.broadcasted_iota(jnp.int32, (1, COLS), 1)
    return jnp.where(position < count, 2.0 * route_row + rank, -1.0)


def slot_matrix(route_row, count):
    slots = lax.broadcasted_iota(jnp.int32, (COLS, COLS), 0).astype(F32)
    hit = slots == jnp.broadcast_to(slot_row(route_row, count), (COLS, COLS))
    return jnp.where(hit, 1.0, 0.0).astype(BF16)


def as_columns(grid, lon, width):
    shape = (LAT, LAT)
    same = lax.broadcasted_iota(jnp.int32, shape, 0) == lax.broadcasted_iota(jnp.int32, shape, 1)
    picked = jnp.where(same, jnp.broadcast_to(grid[lon : lon + 1, :], shape), 0.0)
    return jnp.broadcast_to(jnp.sum(picked, axis=1, keepdims=True), (LAT, width))


def edges_kernel(state, edges):
    edges[0] = state[pl.ds((LON - 1) * ROWS, ROWS), :].astype(BF16)
    edges[1] = state[pl.ds(0, ROWS), :].astype(BF16)
    edges[2] = state[pl.ds(LAT - 1, LON * VARS, stride=LAT), :].astype(BF16)
    edges[3] = state[pl.ds(0, LON * VARS, stride=LAT), :].astype(BF16)


def halo_kernel(edges, halos, send_sem, recv_sem):
    tile, lat, emu = lax.axis_index("tile"), lax.axis_index("lat"), lax.axis_index("emu")
    barrier = pltpu.get_barrier_semaphore()
    tiles = NZ * NY
    east = (lax.rem(tile + 1, tiles), lat, emu)
    west = (lax.rem(tile + tiles - 1, tiles), lat, emu)
    other = (tile, lat, 1 - emu)
    across = (tile, lax.rem(lat + NX - 1 + 2 * emu, NX), 1 - emu)
    for device in (east, west, other, across):
        pl.semaphore_signal(barrier, inc=1, device_id=device, device_id_type=MESH)
    pl.semaphore_wait(barrier, 4)
    copies = []
    for k, (edge, device) in enumerate(((0, east), (1, west), (2 + emu, other), (3 - emu, across))):
        copy = pltpu.make_async_remote_copy(
            src_ref=edges.at[edge], dst_ref=halos.at[edge], send_sem=send_sem.at[k],
            recv_sem=recv_sem.at[k], device_id=device, device_id_type=MESH,
        )
        copy.start()
        copies.append(copy)
    for copy in copies:
        copy.wait()


def step_kernel(state, halos, diff, wind, land, route, count, where, outbound, kept, feats):
    one_hot = slot_matrix(route[...], count[0, 0])
    sub = lax.broadcasted_iota(jnp.int32, (LAT, LEV), 0)
    winds = wind[...]
    lands = land[...].astype(F32)
    keep_south = where[0, 0].astype(F32)
    keep_north = where[0, 1].astype(F32)
    for lon in range(LON):
        gust = 0.5 * as_columns(winds, lon, LEV)
        feats[lon * LAT : (lon + 1) * LAT, VARS * LEV :] = as_columns(lands, lon, LEV).astype(BF16)
        south_rows = halos[2, lon * VARS : (lon + 1) * VARS, :].astype(F32) * keep_south
        north_rows = halos[3, lon * VARS : (lon + 1) * VARS, :].astype(F32) * keep_north
        for v in range(VARS):
            row = lon * ROWS + v * LAT
            mid = state[pl.ds(row, LAT), :]
            if lon < LON - 1:
                right = state[pl.ds(row + ROWS, LAT), :]
            else:
                right = halos[1, v * LAT : (v + 1) * LAT, :].astype(F32)
            if lon > 0:
                left = state[pl.ds(row - ROWS, LAT), :]
            else:
                left = halos[0, v * LAT : (v + 1) * LAT, :].astype(F32)
            up = jnp.where(
                sub == LAT - 1,
                jnp.broadcast_to(north_rows[v : v + 1, :], (LAT, LEV)),
                pltpu.roll(mid, LAT - 1, 0),
            )
            down = jnp.where(
                sub == 0,
                jnp.broadcast_to(south_rows[v : v + 1, :], (LAT, LEV)),
                pltpu.roll(mid, 1, 0),
            )
            spread = right + left + up + down - 4.0 * mid
            moved = mid + diff[v : v + 1, :] * spread - gust * (right - left)
            feats[lon * LAT : (lon + 1) * LAT, v * LEV : (v + 1) * LEV] = moved.astype(BF16)
            if v < OUTV:
                kept[pl.ds((lon * OUTV + v) * LAT, LAT), :] = moved
    for v in range(WORDS):
        rows = jnp.dot(one_hot, feats[:, v * LEV : (v + 1) * LEV], preferred_element_type=F32)
        outbound[v] = rows.astype(BF16).reshape(PEERS, 2, LEV)


def position():
    tile, lat, emu = lax.axis_index("tile"), lax.axis_index("lat"), lax.axis_index("emu")
    return (lax.div(tile, NZ), lax.rem(tile, NZ), lat), emu, tile * NX + lat


def greet_all(me, emu):
    barrier = pltpu.get_barrier_semaphore()

    def one(index, carry):
        tile_to, lat_to = place(lax.rem(index, PLANE), lax.div(index, PLANE), me)
        pl.semaphore_signal(
            barrier, inc=1, device_id=(tile_to, lat_to, emu), device_id_type=MESH
        )
        return carry

    lax.fori_loop(1, PEERS, one, 0)
    pl.semaphore_wait(barrier, PEERS - 1)


def z_of(index):
    half = lax.div(index + 1, 2)
    return NZ // 2 + (2 * lax.rem(index, 2) - 1) * half * (-1)


def dispatch_kernel(outbound, inbound, send_sem, recv_sem, own_sem):
    me, emu, expert = position()
    own = pltpu.make_async_copy(outbound.at[:, expert], inbound.at[:, PEERS - PLANE], own_sem)
    own.start()
    greet_all(me, emu)

    def send(index):
        step = lax.rem(index, PLANE)
        tile_to, lat_to = place(step, z_of(lax.div(index, PLANE)), me)
        return pltpu.make_async_remote_copy(
            src_ref=outbound.at[:, tile_to * NX + lat_to], dst_ref=inbound.at[:, index],
            send_sem=send_sem, recv_sem=recv_sem,
            device_id=(tile_to, lat_to, emu), device_id_type=MESH,
        )

    def start(index, carry):
        send(index).start()
        return carry

    lax.fori_loop(0, PEERS - PLANE, start, 0)
    lax.fori_loop(PEERS - PLANE + 1, PEERS, start, 0)
    pltpu.make_async_remote_copy(
        src_ref=outbound.at[:, pl.ds(0, PEERS - 1)], dst_ref=inbound.at[:, pl.ds(0, PEERS - 1)],
        send_sem=send_sem, recv_sem=recv_sem,
        device_id=(*place(1, 0, me), emu), device_id_type=MESH,
    ).wait()
    own.wait()


def return_kernel(answers, returned, send_sem, recv_sem, own_sem):
    me, emu, expert = position()
    own = pltpu.make_async_copy(answers.at[:, PEERS - PLANE], returned.at[:, expert], own_sem)
    own.start()
    greet_all(me, emu)

    def send(index):
        step = lax.rem(index, PLANE)
        tile_to, lat_to = source(step, z_of(lax.div(index, PLANE)), me)
        return pltpu.make_async_remote_copy(
            src_ref=answers.at[:, index], dst_ref=returned.at[:, expert],
            send_sem=send_sem, recv_sem=recv_sem,
            device_id=(tile_to, lat_to, emu), device_id_type=MESH,
        )

    def start(index, carry):
        send(index).start()
        return carry

    lax.fori_loop(0, PEERS - PLANE, start, 0)
    lax.fori_loop(PEERS - PLANE + 1, PEERS, start, 0)
    pltpu.make_async_remote_copy(
        src_ref=answers.at[:, pl.ds(0, PEERS - 1)], dst_ref=returned.at[:, pl.ds(0, PEERS - 1)],
        send_sem=send_sem, recv_sem=recv_sem,
        device_id=(*place(1, 0, me), emu), device_id_type=MESH,
    ).wait()
    own.wait()


def network_kernel(inbound, w_in, b_in, land_vec, w_hid, b_hid, w_out, answers):
    rows = 2 * PEERS
    taken = jnp.concatenate([inbound[v].reshape(rows, LEV) for v in range(VARS)], axis=1)
    flag = inbound[VARS].reshape(rows, LEV).astype(F32)
    flag = jnp.concatenate([flag] * (HID // LEV), axis=1)
    hidden = jnp.dot(taken, w_in[...], preferred_element_type=F32)
    hidden = jax.nn.silu(hidden + b_in[...] + flag * land_vec[...]).astype(BF16)
    for layer in range(2):
        inner = jnp.dot(hidden, w_hid[layer], preferred_element_type=F32)
        hidden = jax.nn.silu(inner + b_hid[layer : layer + 1, :]).astype(BF16)
    made = jnp.dot(hidden, w_out[...], preferred_element_type=F32).astype(BF16)
    for v in range(OUTV):
        answers[v] = made[:, v * LEV : (v + 1) * LEV].reshape(PEERS, 2, LEV)


def combine_kernel(returned, kept, route, count, out):
    one_hot = slot_matrix(route[...], count[0, 0])
    flat = jnp.concatenate([returned[v].reshape(COLS, LEV) for v in range(OUTV)], axis=1)
    tendency = lax.dot_general(
        one_hot, flat, (((0,), (0,)), ((), ())), preferred_element_type=F32
    )
    for lon in range(LON):
        for v in range(OUTV):
            base = kept[pl.ds((lon * OUTV + v) * LAT, LAT), :]
            added = tendency[lon * LAT : (lon + 1) * LAT, v * LEV : (v + 1) * LEV]
            out[pl.ds(lon * LAT * OUTV + v, LAT, stride=OUTV), :] = base + added


def body(state, diff, wind, land, routes, counts, w_in, b_in, land_vec, w_hid, b_hid, w_out):
    flat_state = jnp.transpose(state, (0, 2, 1, 3)).reshape(LON * ROWS, LEV)
    route = routes.reshape(1, COLS).astype(F32)
    count = counts.reshape(1, 1)
    lat, emu = lax.axis_index("lat"), lax.axis_index("emu")
    south = jnp.where((lat == 0) & (emu == 0), 0, 1)
    north = jnp.where((lat == NX - 1) & (emu == 1), 0, 1)
    where = jnp.stack([south, north]).reshape(1, 2).astype(jnp.int32)
    vmem = pl.BlockSpec(memory_space=pltpu.VMEM)
    smem = pl.BlockSpec(memory_space=pltpu.SMEM)
    hbm = pl.BlockSpec(memory_space=pl.ANY)
    dma = pltpu.SemaphoreType.DMA
    edge = jax.ShapeDtypeStruct((4, ROWS, LEV), BF16)
    features = jax.ShapeDtypeStruct((WORDS, PEERS, 2, LEV), BF16)
    answer = jax.ShapeDtypeStruct((OUTV, PEERS, 2, LEV), BF16)

    def remote(number):
        return pltpu.CompilerParams(
            collective_id=number, has_side_effects=True, vmem_limit_bytes=4 << 20
        )

    def local(size):
        return pltpu.CompilerParams(vmem_limit_bytes=size << 20)

    edges = pl.pallas_call(
        edges_kernel, out_shape=edge, in_specs=[vmem], out_specs=vmem,
        compiler_params=local(4), name="edges",
    )(flat_state)
    halos = pl.pallas_call(
        halo_kernel, out_shape=edge, in_specs=[hbm], out_specs=hbm,
        scratch_shapes=[dma((4,)), dma((4,))],
        compiler_params=remote(0), name="halo",
    )(edges)
    outbound, kept = pl.pallas_call(
        step_kernel,
        out_shape=(features, jax.ShapeDtypeStruct((LON * OUTV * LAT, LEV), F32)),
        in_specs=[vmem, vmem, vmem, vmem, vmem, vmem, smem, smem], out_specs=(vmem, vmem),
        scratch_shapes=[pltpu.VMEM((COLS, WORDS * LEV), BF16)],
        compiler_params=local(8), name="step",
    )(flat_state, halos, diff, wind, land, route, count, where)
    inbound = pl.pallas_call(
        dispatch_kernel, out_shape=features, in_specs=[hbm], out_specs=hbm,
        scratch_shapes=[dma, dma, dma],
        compiler_params=remote(1), name="dispatch",
    )(outbound)
    answers = pl.pallas_call(
        network_kernel, out_shape=answer,
        in_specs=[vmem] * 7, out_specs=vmem,
        compiler_params=local(24), name="network",
    )(inbound, w_in[0], b_in, land_vec, w_hid[0], b_hid[0], w_out[0])
    returned = pl.pallas_call(
        return_kernel, out_shape=answer, in_specs=[hbm], out_specs=hbm,
        scratch_shapes=[dma, dma, dma],
        compiler_params=remote(2), name="give_back",
    )(answers)
    out = pl.pallas_call(
        combine_kernel,
        out_shape=jax.ShapeDtypeStruct((COLS * OUTV, LEV), F32),
        in_specs=[vmem, vmem, vmem, smem],
        out_specs=vmem,
        compiler_params=local(8), name="combine",
    )(returned, kept, route, count)
    return out.reshape(LON, LAT, OUTV, LEV)


def solution(mesh):
    in_specs = (
        P("tile", ("lat", "emu"), None, None),
        P(),
        P("tile", ("lat", "emu")),
        P("tile", ("lat", "emu")),
        P("tile", "lat", "emu", None, None),
        P("tile", "lat", "emu"),
        P(("tile", "lat"), None, None),
        P(("tile", "lat"), None),
        P(("tile", "lat"), None),
        P(("tile", "lat"), None, None, None),
        P(("tile", "lat"), None, None),
        P(("tile", "lat"), None, None),
    )
    out_specs = P("tile", ("lat", "emu"), None, None)
    return jax.shard_map(body, mesh=mesh, in_specs=in_specs, out_specs=out_specs, check_vma=False)
```

```python
import functools

import jax
import jax.numpy as jnp
from jax import lax
from jax.experimental import pallas as pl
from jax.experimental.pallas import tpu as pltpu
from jax.sharding import PartitionSpec as P

MESH = pl.DeviceIdType.MESH
BF16 = jnp.bfloat16
F32 = jnp.float32

NY, NZ, NX = 4, 8, 4
PLANE = NY * NX
PEERS = PLANE * NZ
LON, LAT, VARS, LEV, OUTV = 16, 16, 12, 128, 4
COLS = LON * LAT
ROWS = VARS * LAT
HID = 1024
WORDS = VARS + 1


PIECES = ((0, 80), (80, 128))


def place(step, z_off, me):
    y, z, lat = me
    d_x, d_y = lax.rem(step, NX), lax.div(step, NX)
    tile = lax.rem(y + d_y, NY) * NZ + lax.rem(z + z_off, NZ)
    return tile, lax.rem(lat + d_x, NX)


def source(step, z_off, me):
    y, z, lat = me
    d_x, d_y = lax.rem(step, NX), lax.div(step, NX)
    tile = lax.rem(y + NY - d_y, NY) * NZ + lax.rem(z + NZ - z_off, NZ)
    return tile, lax.rem(lat + NX - d_x, NX)


def slot_row(route_row, count):
    shape = (COLS, COLS)
    first = lax.broadcasted_iota(jnp.int32, shape, 0)
    second = lax.broadcasted_iota(jnp.int32, shape, 1)
    row = jnp.broadcast_to(route_row, shape)
    diagonal = jnp.where(first == second, row, 0.0)
    column = jnp.broadcast_to(jnp.sum(diagonal, axis=1, keepdims=True), shape)
    earlier = (first < second) & (row == column) & (first < count)
    rank = jnp.sum(jnp.where(earlier, 1.0, 0.0), axis=0, keepdims=True)
    position = lax.broadcasted_iota(jnp.int32, (1, COLS), 1)
    return jnp.where(position < count, 2.0 * route_row + rank, -1.0)


def slot_matrix(route_row, count):
    slots = lax.broadcasted_iota(jnp.int32, (COLS, COLS), 0).astype(F32)
    hit = slots == jnp.broadcast_to(slot_row(route_row, count), (COLS, COLS))
    return jnp.where(hit, 1.0, 0.0).astype(BF16)


def as_columns(grid, lon, width):
    shape = (LAT, LAT)
    same = lax.broadcasted_iota(jnp.int32, shape, 0) == lax.broadcasted_iota(jnp.int32, shape, 1)
    picked = jnp.where(same, jnp.broadcast_to(grid[lon : lon + 1, :], shape), 0.0)
    return jnp.broadcast_to(jnp.sum(picked, axis=1, keepdims=True), (LAT, width))


def prepare_kernel(
    state, diff, wind, land, route,
    edges, state_out, diff_out, wind_out, land_out, route_out, sems,
):
    copies = [
        pltpu.make_async_copy(source, target, sems.at[k])
        for k, (source, target) in enumerate(
            ((state, state_out), (diff, diff_out), (wind, wind_out), (land, land_out), (route, route_out))
        )
    ]
    for copy in copies:
        copy.start()
    for copy in copies:
        copy.wait()
    edges[0] = state_out[pl.ds((LON - 1) * ROWS, ROWS), :].astype(BF16)
    edges[1] = state_out[pl.ds(0, ROWS), :].astype(BF16)
    edges[2] = state_out[pl.ds(LAT - 1, LON * VARS, stride=LAT), :].astype(BF16)
    edges[3] = state_out[pl.ds(0, LON * VARS, stride=LAT), :].astype(BF16)


def halo_kernel(edges, halos, send_sem, recv_sem):
    tile, lat, emu = lax.axis_index("tile"), lax.axis_index("lat"), lax.axis_index("emu")
    barrier = pltpu.get_barrier_semaphore()
    tiles = NZ * NY
    east = (lax.rem(tile + 1, tiles), lat, emu)
    west = (lax.rem(tile + tiles - 1, tiles), lat, emu)
    other = (tile, lat, 1 - emu)
    across = (tile, lax.rem(lat + NX - 1 + 2 * emu, NX), 1 - emu)
    for device in (east, west, other, across):
        pl.semaphore_signal(barrier, inc=1, device_id=device, device_id_type=MESH)
    pl.semaphore_wait(barrier, 4)
    copies = []
    for k, (edge, device) in enumerate(((0, east), (1, west), (2 + emu, other), (3 - emu, across))):
        copy = pltpu.make_async_remote_copy(
            src_ref=edges.at[edge], dst_ref=halos.at[edge], send_sem=send_sem.at[k],
            recv_sem=recv_sem.at[k], device_id=device, device_id_type=MESH,
        )
        copy.start()
        copies.append(copy)
    for copy in copies:
        copy.wait()


def step_kernel(state, halos, diff, wind, land, route, count, outbound, kept, feats):
    one_hot = slot_matrix(route[...].astype(F32), count[0, 0])
    sub = lax.broadcasted_iota(jnp.int32, (LAT, LEV), 0)
    winds = wind[...]
    lands = land[...].astype(F32)
    lat, emu = lax.axis_index("lat"), lax.axis_index("emu")
    keep_south = jnp.where((lat == 0) & (emu == 0), 0.0, 1.0).astype(F32)
    keep_north = jnp.where((lat == NX - 1) & (emu == 1), 0.0, 1.0).astype(F32)
    for lon in range(LON):
        gust = 0.5 * as_columns(winds, lon, LEV)
        feats[lon * LAT : (lon + 1) * LAT, VARS * LEV :] = as_columns(lands, lon, LEV).astype(BF16)
        south_rows = halos[2, lon * VARS : (lon + 1) * VARS, :].astype(F32) * keep_south
        north_rows = halos[3, lon * VARS : (lon + 1) * VARS, :].astype(F32) * keep_north
        for v in range(VARS):
            row = lon * ROWS + v * LAT
            mid = state[pl.ds(row, LAT), :]
            if lon < LON - 1:
                right = state[pl.ds(row + ROWS, LAT), :]
            else:
                right = halos[1, v * LAT : (v + 1) * LAT, :].astype(F32)
            if lon > 0:
                left = state[pl.ds(row - ROWS, LAT), :]
            else:
                left = halos[0, v * LAT : (v + 1) * LAT, :].astype(F32)
            up = jnp.where(
                sub == LAT - 1,
                jnp.broadcast_to(north_rows[v : v + 1, :], (LAT, LEV)),
                pltpu.roll(mid, LAT - 1, 0),
            )
            down = jnp.where(
                sub == 0,
                jnp.broadcast_to(south_rows[v : v + 1, :], (LAT, LEV)),
                pltpu.roll(mid, 1, 0),
            )
            spread = right + left + up + down - 4.0 * mid
            moved = mid + diff[v : v + 1, :] * spread - gust * (right - left)
            feats[lon * LAT : (lon + 1) * LAT, v * LEV : (v + 1) * LEV] = moved.astype(BF16)
            if v < OUTV:
                kept[pl.ds((lon * OUTV + v) * LAT, LAT), :] = moved
    for v in range(WORDS):
        rows = jnp.dot(one_hot, feats[:, v * LEV : (v + 1) * LEV], preferred_element_type=F32)
        outbound[v] = rows.astype(BF16).reshape(PEERS, 2, LEV)


def position():
    tile, lat, emu = lax.axis_index("tile"), lax.axis_index("lat"), lax.axis_index("emu")
    return (lax.div(tile, NZ), lax.rem(tile, NZ), lat), emu, tile * NX + lat


def greet_all(me, emu):
    barrier = pltpu.get_barrier_semaphore()

    def one(index, carry):
        tile_to, lat_to = place(lax.rem(index, PLANE), lax.div(index, PLANE), me)
        pl.semaphore_signal(
            barrier, inc=1, device_id=(tile_to, lat_to, emu), device_id_type=MESH
        )
        return carry

    lax.fori_loop(1, PEERS, one, 0)
    pl.semaphore_wait(barrier, PEERS - 1)


def z_of(index):
    half = lax.div(index + 1, 2)
    return NZ // 2 + (2 * lax.rem(index, 2) - 1) * half * (-1)


def network(inbound, span, rows, w_in, b_in, land_vec, w_hid, b_hid, w_out):
    taken = jnp.concatenate([inbound[v, span].reshape(rows, LEV) for v in range(VARS)], axis=1)
    flag = inbound[VARS, span].reshape(rows, LEV).astype(F32)
    flag = jnp.concatenate([flag] * (HID // LEV), axis=1)
    hidden = jnp.dot(taken, w_in[...], preferred_element_type=F32)
    hidden = jax.nn.silu(hidden + b_in[...] + flag * land_vec[...]).astype(BF16)
    for layer in range(2):
        inner = jnp.dot(hidden, w_hid[layer], preferred_element_type=F32)
        hidden = jax.nn.silu(inner + b_hid[layer : layer + 1, :]).astype(BF16)
    return jnp.dot(hidden, w_out[...], preferred_element_type=F32).astype(BF16)


def exchange_kernel(
    outbound, w_in, b_in, land_vec, w_hid, b_hid, w_out, returned,
    inbound, answers, go_send, go_recv, back_send, back_recv, own_sem,
):
    me, emu, expert = position()
    own_slot = PEERS - PLANE
    own = pltpu.make_async_copy(outbound.at[:, expert], inbound.at[:, own_slot], own_sem.at[0])
    own.start()
    greet_all(me, emu)

    def forward(piece, index):
        tile_to, lat_to = place(lax.rem(index, PLANE), z_of(lax.div(index, PLANE)), me)
        return pltpu.make_async_remote_copy(
            src_ref=outbound.at[:, tile_to * NX + lat_to], dst_ref=inbound.at[:, index],
            send_sem=go_send.at[piece], recv_sem=go_recv.at[piece],
            device_id=(tile_to, lat_to, emu), device_id_type=MESH,
        )

    def backward(piece, index):
        tile_to, lat_to = source(lax.rem(index, PLANE), z_of(lax.div(index, PLANE)), me)
        return pltpu.make_async_remote_copy(
            src_ref=answers.at[:, index], dst_ref=returned.at[:, expert],
            send_sem=back_send.at[piece], recv_sem=back_recv.at[piece],
            device_id=(tile_to, lat_to, emu), device_id_type=MESH,
        )

    def start_all(make, piece, first, last):
        def one(index, carry):
            make(piece, index).start()
            return carry

        if first <= own_slot < last:
            lax.fori_loop(first, own_slot, one, 0)
            lax.fori_loop(own_slot + 1, last, one, 0)
        else:
            lax.fori_loop(first, last, one, 0)

    def finish(source_ref, target_ref, send_sem, recv_sem, piece, first, last):
        size = last - first - (1 if first <= own_slot < last else 0)
        pltpu.make_async_remote_copy(
            src_ref=source_ref.at[:, pl.ds(0, size)], dst_ref=target_ref.at[:, pl.ds(0, size)],
            send_sem=send_sem.at[piece], recv_sem=recv_sem.at[piece],
            device_id=(*place(1, 0, me), emu), device_id_type=MESH,
        ).wait()

    for piece, (first, last) in enumerate(PIECES):
        start_all(forward, piece, first, last)
    for piece, (first, last) in enumerate(PIECES):
        finish(outbound, inbound, go_send, go_recv, piece, first, last)
        if first <= own_slot < last:
            own.wait()
        span = slice(first, last)
        made = network(
            inbound, span, 2 * (last - first), w_in, b_in, land_vec, w_hid, b_hid, w_out
        )
        for v in range(OUTV):
            part = made[:, v * LEV : (v + 1) * LEV]
            answers[v, span] = part.reshape(last - first, 2, LEV)
        start_all(backward, piece, first, last)
    mine = pltpu.make_async_copy(answers.at[:, own_slot], returned.at[:, expert], own_sem.at[1])
    mine.start()
    for piece, (first, last) in enumerate(PIECES):
        finish(answers, returned, back_send, back_recv, piece, first, last)
    mine.wait()


def combine_kernel(returned, kept, route, count, out):
    one_hot = slot_matrix(route[...].astype(F32), count[0, 0])
    flat = jnp.concatenate([returned[v].reshape(COLS, LEV) for v in range(OUTV)], axis=1)
    tendency = lax.dot_general(
        one_hot, flat, (((0,), (0,)), ((), ())), preferred_element_type=F32
    )
    for lon in range(LON):
        for v in range(OUTV):
            base = kept[pl.ds((lon * OUTV + v) * LAT, LAT), :]
            added = tendency[lon * LAT : (lon + 1) * LAT, v * LEV : (v + 1) * LEV]
            out[pl.ds(lon * LAT * OUTV + v, LAT, stride=OUTV), :] = base + added


def body(state, diff, wind, land, routes, counts, w_in, b_in, land_vec, w_hid, b_hid, w_out):
    flat_state = jnp.transpose(state, (0, 2, 1, 3)).reshape(LON * ROWS, LEV)
    route = routes.reshape(1, COLS)
    count = counts.reshape(1, 1)
    vmem = pl.BlockSpec(memory_space=pltpu.VMEM)
    smem = pl.BlockSpec(memory_space=pltpu.SMEM)
    hbm = pl.BlockSpec(memory_space=pltpu.HBM)
    anywhere = pl.BlockSpec(memory_space=pl.ANY)
    dma = pltpu.SemaphoreType.DMA
    edge = jax.ShapeDtypeStruct((4, ROWS, LEV), BF16)
    features = jax.ShapeDtypeStruct((WORDS, PEERS, 2, LEV), BF16)
    answer = jax.ShapeDtypeStruct((OUTV, PEERS, 2, LEV), BF16)
    loaded = [jax.ShapeDtypeStruct(x.shape, x.dtype) for x in (flat_state, diff, wind, land, route)]

    def remote(number, size):
        return pltpu.CompilerParams(
            collective_id=number, has_side_effects=True, vmem_limit_bytes=size << 20
        )

    def local(size):
        return pltpu.CompilerParams(vmem_limit_bytes=size << 20)

    def cost(flops, size):
        return pl.CostEstimate(flops=flops, bytes_accessed=size, transcendentals=0)

    edges, flat_state, diff, wind, land, route = pl.pallas_call(
        prepare_kernel, out_shape=[edge] + loaded, in_specs=[hbm] * 5, out_specs=[vmem] * 6,
        scratch_shapes=[dma((5,))], cost_estimate=cost(10**7, 2 * 10**6),
        compiler_params=local(4), name="prepare",
    )(*[pltpu.with_memory_space_constraint(x, pltpu.HBM) for x in (flat_state, diff, wind, land, route)])
    halos = pl.pallas_call(
        halo_kernel, out_shape=edge, in_specs=[anywhere], out_specs=anywhere,
        scratch_shapes=[dma((4,)), dma((4,))], cost_estimate=cost(10**10, 2 * 10**7),
        compiler_params=remote(0, 4), name="halo",
    )(edges)
    outbound, kept = pl.pallas_call(
        step_kernel,
        out_shape=(features, jax.ShapeDtypeStruct((LON * OUTV * LAT, LEV), F32)),
        in_specs=[vmem, vmem, vmem, vmem, vmem, vmem, smem], out_specs=(vmem, vmem),
        scratch_shapes=[pltpu.VMEM((COLS, WORDS * LEV), BF16)], cost_estimate=cost(10**10, 2 * 10**7),
        compiler_params=local(8), name="step",
    )(flat_state, halos, diff, wind, land, route, count)
    returned = pl.pallas_call(
        exchange_kernel, out_shape=answer,
        in_specs=[anywhere] + [vmem] * 6, out_specs=anywhere,
        scratch_shapes=[
            pltpu.VMEM(features.shape, BF16),
            pltpu.VMEM(answer.shape, BF16),
            dma((2,)), dma((2,)), dma((2,)), dma((2,)), dma((2,)),
        ],
        cost_estimate=cost(2 * 10**9, 10**7),
        compiler_params=remote(1, 20), name="exchange",
    )(outbound, w_in[0], b_in, land_vec, w_hid[0], b_hid[0], w_out[0])
    out = pl.pallas_call(
        combine_kernel,
        out_shape=jax.ShapeDtypeStruct((COLS * OUTV, LEV), F32),
        in_specs=[vmem, vmem, vmem, smem],
        out_specs=vmem,
        compiler_params=local(8), name="combine",
    )(returned, kept, route, count)
    return out.reshape(LON, LAT, OUTV, LEV)


def solution(mesh):
    in_specs = (
        P("tile", ("lat", "emu"), None, None),
        P(),
        P("tile", ("lat", "emu")),
        P("tile", ("lat", "emu")),
        P("tile", "lat", "emu", None, None),
        P("tile", "lat", "emu"),
        P(("tile", "lat"), None, None),
        P(("tile", "lat"), None),
        P(("tile", "lat"), None),
        P(("tile", "lat"), None, None, None),
        P(("tile", "lat"), None, None),
        P(("tile", "lat"), None, None),
    )
    out_specs = P("tile", ("lat", "emu"), None, None)
    return jax.shard_map(body, mesh=mesh, in_specs=in_specs, out_specs=out_specs, check_vma=False)
```

```python
import functools

import jax
import jax.numpy as jnp
from jax import lax
from jax.experimental import pallas as pl
from jax.experimental.pallas import tpu as pltpu
from jax.sharding import PartitionSpec as P

MESH = pl.DeviceIdType.MESH
BF16 = jnp.bfloat16
F32 = jnp.float32

NY, NZ, NX = 4, 8, 4
PLANE = NY * NX
PEERS = PLANE * NZ
LON, LAT, VARS, LEV, OUTV = 16, 16, 12, 128, 4
COLS = LON * LAT
ROWS = VARS * LAT
HID = 1024
WORDS = VARS + 1


PIECES = ((0, 80), (80, 128))


def place(step, z_off, me):
    y, z, lat = me
    d_x, d_y = lax.rem(step, NX), lax.div(step, NX)
    tile = lax.rem(y + d_y, NY) * NZ + lax.rem(z + z_off, NZ)
    return tile, lax.rem(lat + d_x, NX)


def source(step, z_off, me):
    y, z, lat = me
    d_x, d_y = lax.rem(step, NX), lax.div(step, NX)
    tile = lax.rem(y + NY - d_y, NY) * NZ + lax.rem(z + NZ - z_off, NZ)
    return tile, lax.rem(lat + NX - d_x, NX)


def slot_row(route_row, count):
    shape = (COLS, COLS)
    first = lax.broadcasted_iota(jnp.int32, shape, 0)
    second = lax.broadcasted_iota(jnp.int32, shape, 1)
    row = jnp.broadcast_to(route_row, shape)
    diagonal = jnp.where(first == second, row, 0.0)
    column = jnp.broadcast_to(jnp.sum(diagonal, axis=1, keepdims=True), shape)
    earlier = (first < second) & (row == column) & (first < count)
    rank = jnp.sum(jnp.where(earlier, 1.0, 0.0), axis=0, keepdims=True)
    position = lax.broadcasted_iota(jnp.int32, (1, COLS), 1)
    return jnp.where(position < count, 2.0 * route_row + rank, -1.0)


def slot_matrix(route_row, count):
    slots = lax.broadcasted_iota(jnp.int32, (COLS, COLS), 0).astype(F32)
    hit = slots == jnp.broadcast_to(slot_row(route_row, count), (COLS, COLS))
    return jnp.where(hit, 1.0, 0.0).astype(BF16)


def as_columns(row, width):
    shape = (LAT, LAT)
    same = lax.broadcasted_iota(jnp.int32, shape, 0) == lax.broadcasted_iota(jnp.int32, shape, 1)
    picked = jnp.where(same, jnp.broadcast_to(row, shape), 0.0)
    return jnp.broadcast_to(jnp.sum(picked, axis=1, keepdims=True), (LAT, width))


def prepare_kernel(
    state, diff, wind, land, route,
    edges, state_out, diff_out, wind_out, land_out, route_out, sems,
):
    copies = [
        pltpu.make_async_copy(source, target, sems.at[k])
        for k, (source, target) in enumerate(
            ((state, state_out), (diff, diff_out), (wind, wind_out), (land, land_out), (route, route_out))
        )
    ]
    for copy in copies:
        copy.start()
    for copy in copies:
        copy.wait()
    edges[0] = state_out[pl.ds((LON - 1) * ROWS, ROWS), :].astype(BF16)
    edges[1] = state_out[pl.ds(0, ROWS), :].astype(BF16)
    edges[2] = state_out[pl.ds(LAT - 1, LON * VARS, stride=LAT), :].astype(BF16)
    edges[3] = state_out[pl.ds(0, LON * VARS, stride=LAT), :].astype(BF16)


def halo_kernel(edges, halos, send_sem, recv_sem):
    tile, lat, emu = lax.axis_index("tile"), lax.axis_index("lat"), lax.axis_index("emu")
    barrier = pltpu.get_barrier_semaphore()
    tiles = NZ * NY
    east = (lax.rem(tile + 1, tiles), lat, emu)
    west = (lax.rem(tile + tiles - 1, tiles), lat, emu)
    other = (tile, lat, 1 - emu)
    across = (tile, lax.rem(lat + NX - 1 + 2 * emu, NX), 1 - emu)
    for device in (east, west, other, across):
        pl.semaphore_signal(barrier, inc=1, device_id=device, device_id_type=MESH)
    pl.semaphore_wait(barrier, 4)
    copies = []
    for k, (edge, device) in enumerate(((0, east), (1, west), (2 + emu, other), (3 - emu, across))):
        copy = pltpu.make_async_remote_copy(
            src_ref=edges.at[edge], dst_ref=halos.at[edge], send_sem=send_sem.at[k],
            recv_sem=recv_sem.at[k], device_id=device, device_id_type=MESH,
        )
        copy.start()
        copies.append(copy)
    for copy in copies:
        copy.wait()


def advance(
    state, halos, diff, wind, land, route, count, lat, emu, outbound, kept, feats, sides,
):
    one_hot = slot_matrix(route[...].astype(F32), count[0, 0])
    sub = lax.broadcasted_iota(jnp.int32, (LAT, LEV), 0)
    sides[0] = halos[2].astype(F32) * jnp.where((lat == 0) & (emu == 0), 0.0, 1.0).astype(F32)
    sides[1] = halos[3].astype(F32) * jnp.where((lat == NX - 1) & (emu == 1), 0.0, 1.0).astype(F32)

    def one(lon, carry):
        gust = 0.5 * as_columns(wind[pl.ds(lon, 1), :], LEV)
        place_of = pl.ds(pl.multiple_of(lon * LAT, LAT), LAT)
        surface = as_columns(land[pl.ds(lon, 1), :].astype(F32), LEV)
        feats[place_of, VARS * LEV :] = surface.astype(BF16)
        here = lon * ROWS
        east = jnp.minimum(lon + 1, LON - 1) * ROWS
        west = jnp.maximum(lon - 1, 0) * ROWS
        for v in range(VARS):
            inner = slice(v * LAT, (v + 1) * LAT)
            mid = state[pl.ds(pl.multiple_of(here + v * LAT, LAT), LAT), :]
            right = state[pl.ds(pl.multiple_of(east + v * LAT, LAT), LAT), :]
            left = state[pl.ds(pl.multiple_of(west + v * LAT, LAT), LAT), :]
            right = jnp.where(lon == LON - 1, halos[1, inner, :].astype(F32), right)
            left = jnp.where(lon == 0, halos[0, inner, :].astype(F32), left)
            south = jnp.broadcast_to(sides[0, pl.ds(lon * VARS + v, 1), :], (LAT, LEV))
            north = jnp.broadcast_to(sides[1, pl.ds(lon * VARS + v, 1), :], (LAT, LEV))
            up = jnp.where(sub == LAT - 1, north, pltpu.roll(mid, LAT - 1, 0))
            down = jnp.where(sub == 0, south, pltpu.roll(mid, 1, 0))
            spread = right + left + up + down - 4.0 * mid
            moved = mid + diff[v : v + 1, :] * spread - gust * (right - left)
            feats[place_of, v * LEV : (v + 1) * LEV] = moved.astype(BF16)
            if v < OUTV:
                kept[pl.ds(pl.multiple_of((lon * OUTV + v) * LAT, LAT), LAT), :] = moved
        return carry

    lax.fori_loop(0, LON, one, 0)
    for v in range(WORDS):
        rows = jnp.dot(one_hot, feats[:, v * LEV : (v + 1) * LEV], preferred_element_type=F32)
        outbound[v] = rows.astype(BF16).reshape(PEERS, 2, LEV)


def position():
    tile, lat, emu = lax.axis_index("tile"), lax.axis_index("lat"), lax.axis_index("emu")
    return (lax.div(tile, NZ), lax.rem(tile, NZ), lat), emu, tile * NX + lat


def greet_all(barrier, me, emu):
    def one(index, carry):
        tile_to, lat_to = place(lax.rem(index, PLANE), lax.div(index, PLANE), me)
        pl.semaphore_signal(
            barrier, inc=1, device_id=(tile_to, lat_to, emu), device_id_type=MESH
        )
        return carry

    lax.fori_loop(1, PEERS, one, 0)


def z_of(index):
    half = lax.div(index + 1, 2)
    return NZ // 2 + (2 * lax.rem(index, 2) - 1) * half * (-1)


def network(inbound, span, rows, w_in, b_in, land_vec, w_hid, b_hid, w_out):
    taken = jnp.concatenate([inbound[v, span].reshape(rows, LEV) for v in range(VARS)], axis=1)
    flag = inbound[VARS, span].reshape(rows, LEV).astype(F32)
    flag = jnp.concatenate([flag] * (HID // LEV), axis=1)
    hidden = jnp.dot(taken, w_in[...], preferred_element_type=F32)
    hidden = jax.nn.silu(hidden + b_in[...] + flag * land_vec[...]).astype(BF16)
    for layer in range(2):
        inner = jnp.dot(hidden, w_hid[layer], preferred_element_type=F32)
        hidden = jax.nn.silu(inner + b_hid[layer : layer + 1, :]).astype(BF16)
    return jnp.dot(hidden, w_out[...], preferred_element_type=F32).astype(BF16)


def exchange_kernel(
    state, halos, diff, wind, land, route, count,
    w_in_hbm, b_in, land_vec, w_hid_hbm, b_hid, w_out_hbm, returned, kept,
    outbound, inbound, answers, feats, sides, w_in, w_hid, w_out,
    go_send, go_recv, back_send, back_recv, own_sem, weight_sem,
):
    me, emu, expert = position()
    own_slot = PEERS - PLANE
    barrier = pltpu.get_barrier_semaphore()
    greet_all(barrier, me, emu)
    weights = [
        pltpu.make_async_copy(w_in_hbm, w_in, weight_sem.at[0]),
        pltpu.make_async_copy(w_hid_hbm, w_hid, weight_sem.at[1]),
        pltpu.make_async_copy(w_out_hbm, w_out, weight_sem.at[2]),
    ]
    for copy in weights:
        copy.start()
    advance(
        state, halos, diff, wind, land, route, count, me[2], emu, outbound, kept, feats, sides
    )
    own = pltpu.make_async_copy(outbound.at[:, expert], inbound.at[:, own_slot], own_sem.at[0])
    own.start()
    pl.semaphore_wait(barrier, PEERS - 1)

    def forward(piece, index):
        tile_to, lat_to = place(lax.rem(index, PLANE), z_of(lax.div(index, PLANE)), me)
        return pltpu.make_async_remote_copy(
            src_ref=outbound.at[:, tile_to * NX + lat_to], dst_ref=inbound.at[:, index],
            send_sem=go_send.at[piece], recv_sem=go_recv.at[piece],
            device_id=(tile_to, lat_to, emu), device_id_type=MESH,
        )

    def backward(piece, index):
        tile_to, lat_to = source(lax.rem(index, PLANE), z_of(lax.div(index, PLANE)), me)
        return pltpu.make_async_remote_copy(
            src_ref=answers.at[:, index], dst_ref=returned.at[:, expert],
            send_sem=back_send.at[piece], recv_sem=back_recv.at[piece],
            device_id=(tile_to, lat_to, emu), device_id_type=MESH,
        )

    def start_all(make, piece, first, last):
        def one(index, carry):
            make(piece, index).start()
            return carry

        if first <= own_slot < last:
            lax.fori_loop(first, own_slot, one, 0)
            lax.fori_loop(own_slot + 1, last, one, 0)
        else:
            lax.fori_loop(first, last, one, 0)

    def finish(source_ref, target_ref, send_sem, recv_sem, piece, first, last):
        size = last - first - (1 if first <= own_slot < last else 0)
        pltpu.make_async_remote_copy(
            src_ref=source_ref.at[:, pl.ds(0, size)], dst_ref=target_ref.at[:, pl.ds(0, size)],
            send_sem=send_sem.at[piece], recv_sem=recv_sem.at[piece],
            device_id=(*place(1, 0, me), emu), device_id_type=MESH,
        ).wait()

    for piece, (first, last) in enumerate(PIECES):
        start_all(forward, piece, first, last)
    for piece, (first, last) in enumerate(PIECES):
        finish(outbound, inbound, go_send, go_recv, piece, first, last)
        if piece == 0:
            for copy in weights:
                copy.wait()
        if first <= own_slot < last:
            own.wait()
        span = slice(first, last)
        made = network(
            inbound, span, 2 * (last - first), w_in, b_in, land_vec, w_hid, b_hid, w_out
        )
        for v in range(OUTV):
            part = made[:, v * LEV : (v + 1) * LEV]
            answers[v, span] = part.reshape(last - first, 2, LEV)
        start_all(backward, piece, first, last)
    mine = pltpu.make_async_copy(answers.at[:, own_slot], returned.at[:, expert], own_sem.at[1])
    mine.start()
    for piece, (first, last) in enumerate(PIECES):
        finish(answers, returned, back_send, back_recv, piece, first, last)
    mine.wait()


def combine_kernel(returned, kept, route, count, out):
    one_hot = slot_matrix(route[...].astype(F32), count[0, 0])
    flat = jnp.concatenate([returned[v].reshape(COLS, LEV) for v in range(OUTV)], axis=1)
    tendency = lax.dot_general(
        one_hot, flat, (((0,), (0,)), ((), ())), preferred_element_type=F32
    )
    for lon in range(LON):
        for v in range(OUTV):
            base = kept[pl.ds((lon * OUTV + v) * LAT, LAT), :]
            added = tendency[lon * LAT : (lon + 1) * LAT, v * LEV : (v + 1) * LEV]
            out[pl.ds(lon * LAT * OUTV + v, LAT, stride=OUTV), :] = base + added


def body(state, diff, wind, land, routes, counts, w_in, b_in, land_vec, w_hid, b_hid, w_out):
    flat_state = jnp.transpose(state, (0, 2, 1, 3)).reshape(LON * ROWS, LEV)
    route = routes.reshape(1, COLS)
    count = counts.reshape(1, 1)
    vmem = pl.BlockSpec(memory_space=pltpu.VMEM)
    smem = pl.BlockSpec(memory_space=pltpu.SMEM)
    hbm = pl.BlockSpec(memory_space=pltpu.HBM)
    anywhere = pl.BlockSpec(memory_space=pl.ANY)
    dma = pltpu.SemaphoreType.DMA
    edge = jax.ShapeDtypeStruct((4, ROWS, LEV), BF16)
    features = jax.ShapeDtypeStruct((WORDS, PEERS, 2, LEV), BF16)
    answer = jax.ShapeDtypeStruct((OUTV, PEERS, 2, LEV), BF16)
    loaded = [jax.ShapeDtypeStruct(x.shape, x.dtype) for x in (flat_state, diff, wind, land, route)]

    def remote(number, size):
        return pltpu.CompilerParams(
            collective_id=number, has_side_effects=True, vmem_limit_bytes=size << 20
        )

    def local(size):
        return pltpu.CompilerParams(vmem_limit_bytes=size << 20)

    def cost(flops, size):
        return pl.CostEstimate(flops=flops, bytes_accessed=size, transcendentals=0)

    edges, flat_state, diff, wind, land, route = pl.pallas_call(
        prepare_kernel, out_shape=[edge] + loaded, in_specs=[hbm] * 5, out_specs=[vmem] * 6,
        scratch_shapes=[dma((5,))], cost_estimate=cost(10**7, 2 * 10**6),
        compiler_params=local(4), name="prepare",
    )(*[pltpu.with_memory_space_constraint(x, pltpu.HBM) for x in (flat_state, diff, wind, land, route)])
    halos = pl.pallas_call(
        halo_kernel, out_shape=edge, in_specs=[anywhere], out_specs=anywhere,
        scratch_shapes=[dma((4,)), dma((4,))], cost_estimate=cost(10**10, 2 * 10**7),
        compiler_params=remote(0, 4), name="halo",
    )(edges)
    held = [pltpu.with_memory_space_constraint(w[0], pltpu.HBM) for w in (w_in, w_hid, w_out)]
    returned, kept = pl.pallas_call(
        exchange_kernel,
        out_shape=(answer, jax.ShapeDtypeStruct((LON * OUTV * LAT, LEV), F32)),
        in_specs=[vmem] * 6 + [smem, hbm, vmem, vmem, hbm, vmem, hbm],
        out_specs=(anywhere, vmem),
        scratch_shapes=[
            pltpu.VMEM(features.shape, BF16),
            pltpu.VMEM(features.shape, BF16),
            pltpu.VMEM(answer.shape, BF16),
            pltpu.VMEM((COLS, WORDS * LEV), BF16),
            pltpu.VMEM((2, ROWS, LEV), F32),
            pltpu.VMEM(held[0].shape, BF16),
            pltpu.VMEM(held[1].shape, BF16),
            pltpu.VMEM(held[2].shape, BF16),
            dma((2,)), dma((2,)), dma((2,)), dma((2,)), dma((2,)), dma((3,)),
        ],
        cost_estimate=cost(2 * 10**9, 10**7),
        compiler_params=remote(1, 32), name="exchange",
    )(flat_state, halos, diff, wind, land, route, count, held[0], b_in, land_vec, held[1], b_hid[0], held[2])
    out = pl.pallas_call(
        combine_kernel,
        out_shape=jax.ShapeDtypeStruct((COLS * OUTV, LEV), F32),
        in_specs=[vmem, vmem, vmem, smem],
        out_specs=vmem,
        compiler_params=local(8), name="combine",
    )(returned, kept, route, count)
    return out.reshape(LON, LAT, OUTV, LEV)


def solution(mesh):
    in_specs = (
        P("tile", ("lat", "emu"), None, None),
        P(),
        P("tile", ("lat", "emu")),
        P("tile", ("lat", "emu")),
        P("tile", "lat", "emu", None, None),
        P("tile", "lat", "emu"),
        P(("tile", "lat"), None, None),
        P(("tile", "lat"), None),
        P(("tile", "lat"), None),
        P(("tile", "lat"), None, None, None),
        P(("tile", "lat"), None, None),
        P(("tile", "lat"), None, None),
    )
    out_specs = P("tile", ("lat", "emu"), None, None)
    return jax.shard_map(body, mesh=mesh, in_specs=in_specs, out_specs=out_specs, check_vma=False)
```

```python
import functools

import jax
import jax.numpy as jnp
from jax import lax
from jax.experimental import pallas as pl
from jax.experimental.pallas import tpu as pltpu
from jax.sharding import PartitionSpec as P

MESH = pl.DeviceIdType.MESH
BF16 = jnp.bfloat16
F32 = jnp.float32

NY, NZ, NX = 4, 8, 4
PLANE = NY * NX
PEERS = PLANE * NZ
LON, LAT, VARS, LEV, OUTV = 16, 16, 12, 128, 4
COLS = LON * LAT
ROWS = VARS * LAT
HID = 1024
WORDS = VARS + 1


PIECES = ((0, 80), (80, 128))


def place(step, z_off, me):
    y, z, lat = me
    d_x, d_y = lax.rem(step, NX), lax.div(step, NX)
    tile = lax.rem(y + d_y, NY) * NZ + lax.rem(z + z_off, NZ)
    return tile, lax.rem(lat + d_x, NX)


def source(step, z_off, me):
    y, z, lat = me
    d_x, d_y = lax.rem(step, NX), lax.div(step, NX)
    tile = lax.rem(y + NY - d_y, NY) * NZ + lax.rem(z + NZ - z_off, NZ)
    return tile, lax.rem(lat + NX - d_x, NX)


def slot_row(route_row, count):
    shape = (COLS, COLS)
    first = lax.broadcasted_iota(jnp.int32, shape, 0)
    second = lax.broadcasted_iota(jnp.int32, shape, 1)
    row = jnp.broadcast_to(route_row, shape)
    diagonal = jnp.where(first == second, row, 0.0)
    column = jnp.broadcast_to(jnp.sum(diagonal, axis=1, keepdims=True), shape)
    earlier = (first < second) & (row == column) & (first < count)
    rank = jnp.sum(jnp.where(earlier, 1.0, 0.0), axis=0, keepdims=True)
    position = lax.broadcasted_iota(jnp.int32, (1, COLS), 1)
    return jnp.where(position < count, 2.0 * route_row + rank, -1.0)


def slot_matrix(route_row, count):
    slots = lax.broadcasted_iota(jnp.int32, (COLS, COLS), 0).astype(F32)
    hit = slots == jnp.broadcast_to(slot_row(route_row, count), (COLS, COLS))
    return jnp.where(hit, 1.0, 0.0).astype(BF16)


def as_columns(row, width):
    shape = (LAT, LAT)
    same = lax.broadcasted_iota(jnp.int32, shape, 0) == lax.broadcasted_iota(jnp.int32, shape, 1)
    picked = jnp.where(same, jnp.broadcast_to(row, shape), 0.0)
    return jnp.broadcast_to(jnp.sum(picked, axis=1, keepdims=True), (LAT, width))


def advance(state, halos, diff, wind, land, one_hot, lat, emu, outbound, kept, feats, sides):
    sub = lax.broadcasted_iota(jnp.int32, (LAT, LEV), 0)
    sides[0] = halos[2].astype(F32) * jnp.where((lat == 0) & (emu == 0), 0.0, 1.0).astype(F32)
    sides[1] = halos[3].astype(F32) * jnp.where((lat == NX - 1) & (emu == 1), 0.0, 1.0).astype(F32)

    def one(lon, carry):
        gust = 0.5 * as_columns(wind[pl.ds(lon, 1), :], LEV)
        place_of = pl.ds(pl.multiple_of(lon * LAT, LAT), LAT)
        surface = as_columns(land[pl.ds(lon, 1), :].astype(F32), LEV)
        feats[place_of, VARS * LEV :] = surface.astype(BF16)
        here = lon * ROWS
        east = jnp.minimum(lon + 1, LON - 1) * ROWS
        west = jnp.maximum(lon - 1, 0) * ROWS
        for v in range(VARS):
            inner = slice(v * LAT, (v + 1) * LAT)
            mid = state[pl.ds(pl.multiple_of(here + v * LAT, LAT), LAT), :]
            right = state[pl.ds(pl.multiple_of(east + v * LAT, LAT), LAT), :]
            left = state[pl.ds(pl.multiple_of(west + v * LAT, LAT), LAT), :]
            right = jnp.where(lon == LON - 1, halos[1, inner, :].astype(F32), right)
            left = jnp.where(lon == 0, halos[0, inner, :].astype(F32), left)
            south = jnp.broadcast_to(sides[0, pl.ds(lon * VARS + v, 1), :], (LAT, LEV))
            north = jnp.broadcast_to(sides[1, pl.ds(lon * VARS + v, 1), :], (LAT, LEV))
            up = jnp.where(sub == LAT - 1, north, pltpu.roll(mid, LAT - 1, 0))
            down = jnp.where(sub == 0, south, pltpu.roll(mid, 1, 0))
            spread = right + left + up + down - 4.0 * mid
            moved = mid + diff[v : v + 1, :] * spread - gust * (right - left)
            feats[place_of, v * LEV : (v + 1) * LEV] = moved.astype(BF16)
            if v < OUTV:
                kept[pl.ds(pl.multiple_of((lon * OUTV + v) * LAT, LAT), LAT), :] = moved
        return carry

    lax.fori_loop(0, LON, one, 0)
    for v in range(WORDS):
        rows = jnp.dot(one_hot[...], feats[:, v * LEV : (v + 1) * LEV], preferred_element_type=F32)
        outbound[v] = rows.astype(BF16).reshape(PEERS, 2, LEV)


def position():
    tile, lat, emu = lax.axis_index("tile"), lax.axis_index("lat"), lax.axis_index("emu")
    return (lax.div(tile, NZ), lax.rem(tile, NZ), lat), emu, tile * NX + lat


def z_of(index):
    half = lax.div(index + 1, 2)
    return NZ // 2 + (2 * lax.rem(index, 2) - 1) * half * (-1)


def network(inbound, span, rows, w_in, b_in, land_vec, w_hid, b_hid, w_out):
    taken = jnp.concatenate([inbound[v, span].reshape(rows, LEV) for v in range(VARS)], axis=1)
    flag = inbound[VARS, span].reshape(rows, LEV).astype(F32)
    flag = jnp.concatenate([flag] * (HID // LEV), axis=1)
    hidden = jnp.dot(taken, w_in[...], preferred_element_type=F32)
    hidden = jax.nn.silu(hidden + b_in[...] + flag * land_vec[...]).astype(BF16)
    for layer in range(2):
        inner = jnp.dot(hidden, w_hid[layer], preferred_element_type=F32)
        hidden = jax.nn.silu(inner + b_hid[layer : layer + 1, :]).astype(BF16)
    return jnp.dot(hidden, w_out[...], preferred_element_type=F32).astype(BF16)


def exchange_kernel(
    state_hbm, diff_hbm, wind_hbm, land_hbm, route_hbm, count,
    w_in_hbm, b_in_hbm, land_vec_hbm, w_hid_hbm, b_hid_hbm, w_out_hbm, returned, kept,
    state, diff, wind, land, route, edges, halos, one_hot,
    outbound, inbound, answers, feats, sides, w_in, b_in, land_vec, w_hid, b_hid, w_out,
    edge_send, edge_recv, go_send, go_recv, back_send, back_recv, own_sem, load_sem, weight_sem,
    plane_sem, all_sem,
):
    me, emu, expert = position()
    y, z, lat = me
    tile, tiles = y * NZ + z, NY * NZ
    own_slot = PEERS - PLANE

    east = (lax.rem(tile + 1, tiles), lat, emu)
    west = (lax.rem(tile + tiles - 1, tiles), lat, emu)
    other = (tile, lat, 1 - emu)
    across = (tile, lax.rem(lat + NX - 1 + 2 * emu, NX), 1 - emu)
    x_line = [(tile, lax.rem(lat + d, NX), emu) for d in range(1, NX)]
    y_line = [(lax.rem(y + d, NY) * NZ + z, lat, emu) for d in range(1, NY)]
    z_line = [(y * NZ + lax.rem(z + d, NZ), lat, emu) for d in range(1, NZ)]
    greeted = [east, west, other, across] + x_line + y_line + z_line
    barrier = pltpu.get_barrier_semaphore()
    for device in greeted:
        pl.semaphore_signal(barrier, inc=1, device_id=device, device_id_type=MESH)

    def copies_of(pairs, sems):
        made = [pltpu.make_async_copy(a, b, sems.at[k]) for k, (a, b) in enumerate(pairs)]
        for copy in made:
            copy.start()
        return made

    loads = copies_of(
        ((state_hbm, state), (diff_hbm, diff), (wind_hbm, wind), (land_hbm, land), (route_hbm, route)),
        load_sem,
    )
    weights = copies_of(
        (
            (w_in_hbm, w_in), (b_in_hbm, b_in), (land_vec_hbm, land_vec),
            (w_hid_hbm, w_hid), (b_hid_hbm, b_hid), (w_out_hbm, w_out),
        ),
        weight_sem,
    )
    for copy in loads:
        copy.wait()

    edges[0] = state[pl.ds((LON - 1) * ROWS, ROWS), :].astype(BF16)
    edges[1] = state[pl.ds(0, ROWS), :].astype(BF16)
    edges[2] = state[pl.ds(LAT - 1, LON * VARS, stride=LAT), :].astype(BF16)
    edges[3] = state[pl.ds(0, LON * VARS, stride=LAT), :].astype(BF16)
    pl.semaphore_wait(barrier, len(greeted))
    sent = []
    for k, (edge, device) in enumerate(((0, east), (1, west), (2 + emu, other), (3 - emu, across))):
        copy = pltpu.make_async_remote_copy(
            src_ref=edges.at[edge], dst_ref=halos.at[edge], send_sem=edge_send.at[k],
            recv_sem=edge_recv.at[k], device_id=device, device_id_type=MESH,
        )
        copy.start()
        sent.append(copy)
    for device in y_line:
        pl.semaphore_signal(plane_sem, inc=1, device_id=device, device_id_type=MESH)
    one_hot[...] = slot_matrix(route[...].astype(F32), count[0, 0])
    pl.semaphore_wait(plane_sem, len(y_line))
    for device in z_line:
        pl.semaphore_signal(all_sem, inc=1, device_id=device, device_id_type=MESH)
    for copy in sent:
        copy.wait()
    advance(state, halos, diff, wind, land, one_hot, lat, emu, outbound, kept, feats, sides)
    own = pltpu.make_async_copy(outbound.at[:, expert], inbound.at[:, own_slot], own_sem.at[0])
    own.start()
    pl.semaphore_wait(all_sem, len(z_line))

    def forward(piece, index):
        tile_to, lat_to = place(lax.rem(index, PLANE), z_of(lax.div(index, PLANE)), me)
        return pltpu.make_async_remote_copy(
            src_ref=outbound.at[:, tile_to * NX + lat_to], dst_ref=inbound.at[:, index],
            send_sem=go_send.at[piece], recv_sem=go_recv.at[piece],
            device_id=(tile_to, lat_to, emu), device_id_type=MESH,
        )

    def backward(piece, index):
        tile_to, lat_to = source(lax.rem(index, PLANE), z_of(lax.div(index, PLANE)), me)
        return pltpu.make_async_remote_copy(
            src_ref=answers.at[:, index], dst_ref=returned.at[:, expert],
            send_sem=back_send.at[piece], recv_sem=back_recv.at[piece],
            device_id=(tile_to, lat_to, emu), device_id_type=MESH,
        )

    def start_all(make, piece, first, last):
        def one(index, carry):
            make(piece, index).start()
            return carry

        if first <= own_slot < last:
            lax.fori_loop(first, own_slot, one, 0)
            lax.fori_loop(own_slot + 1, last, one, 0)
        else:
            lax.fori_loop(first, last, one, 0)

    def finish(source_ref, target_ref, send_sem, recv_sem, piece, first, last):
        size = last - first - (1 if first <= own_slot < last else 0)
        pltpu.make_async_remote_copy(
            src_ref=source_ref.at[:, pl.ds(0, size)], dst_ref=target_ref.at[:, pl.ds(0, size)],
            send_sem=send_sem.at[piece], recv_sem=recv_sem.at[piece],
            device_id=(*place(1, 0, me), emu), device_id_type=MESH,
        ).wait()

    for piece, (first, last) in enumerate(PIECES):
        start_all(forward, piece, first, last)
    for piece, (first, last) in enumerate(PIECES):
        finish(outbound, inbound, go_send, go_recv, piece, first, last)
        if piece == 0:
            for copy in weights:
                copy.wait()
        if first <= own_slot < last:
            own.wait()
        span = slice(first, last)
        made = network(
            inbound, span, 2 * (last - first), w_in, b_in, land_vec, w_hid, b_hid, w_out
        )
        for v in range(OUTV):
            part = made[:, v * LEV : (v + 1) * LEV]
            answers[v, span] = part.reshape(last - first, 2, LEV)
        start_all(backward, piece, first, last)
    mine = pltpu.make_async_copy(answers.at[:, own_slot], returned.at[:, expert], own_sem.at[1])
    mine.start()
    for piece, (first, last) in enumerate(PIECES):
        finish(answers, returned, back_send, back_recv, piece, first, last)
    mine.wait()


def combine_kernel(returned, kept, route, count, out):
    one_hot = slot_matrix(route[...].astype(F32), count[0, 0])
    flat = jnp.concatenate([returned[v].reshape(COLS, LEV) for v in range(OUTV)], axis=1)
    tendency = lax.dot_general(
        one_hot, flat, (((0,), (0,)), ((), ())), preferred_element_type=F32
    )
    for lon in range(LON):
        for v in range(OUTV):
            base = kept[pl.ds((lon * OUTV + v) * LAT, LAT), :]
            added = tendency[lon * LAT : (lon + 1) * LAT, v * LEV : (v + 1) * LEV]
            out[pl.ds(lon * LAT * OUTV + v, LAT, stride=OUTV), :] = base + added


def body(state, diff, wind, land, routes, counts, w_in, b_in, land_vec, w_hid, b_hid, w_out):
    flat_state = jnp.transpose(state, (0, 2, 1, 3)).reshape(LON * ROWS, LEV)
    route = routes.reshape(1, COLS)
    count = counts.reshape(1, 1)
    vmem = pl.BlockSpec(memory_space=pltpu.VMEM)
    smem = pl.BlockSpec(memory_space=pltpu.SMEM)
    hbm = pl.BlockSpec(memory_space=pltpu.HBM)
    anywhere = pl.BlockSpec(memory_space=pl.ANY)
    dma = pltpu.SemaphoreType.DMA
    features = jax.ShapeDtypeStruct((WORDS, PEERS, 2, LEV), BF16)
    answer = jax.ShapeDtypeStruct((OUTV, PEERS, 2, LEV), BF16)

    def local(size):
        return pltpu.CompilerParams(vmem_limit_bytes=size << 20)

    def held(*arrays):
        return [pltpu.with_memory_space_constraint(x, pltpu.HBM) for x in arrays]

    inputs = held(flat_state, diff, wind, land, route)
    params = held(w_in[0], b_in, land_vec, w_hid[0], b_hid[0], w_out[0])
    returned, kept = pl.pallas_call(
        exchange_kernel,
        out_shape=(answer, jax.ShapeDtypeStruct((LON * OUTV * LAT, LEV), F32)),
        in_specs=[hbm] * 5 + [smem] + [hbm] * 6,
        out_specs=(anywhere, vmem),
        scratch_shapes=[pltpu.VMEM(x.shape, x.dtype) for x in inputs]
        + [
            pltpu.VMEM((4, ROWS, LEV), BF16),
            pltpu.VMEM((4, ROWS, LEV), BF16),
            pltpu.VMEM((COLS, COLS), BF16),
            pltpu.VMEM(features.shape, BF16),
            pltpu.VMEM(features.shape, BF16),
            pltpu.VMEM(answer.shape, BF16),
            pltpu.VMEM((COLS, WORDS * LEV), BF16),
            pltpu.VMEM((2, ROWS, LEV), F32),
        ]
        + [pltpu.VMEM(x.shape, x.dtype) for x in params]
        + [
            dma((4,)), dma((4,)), dma((2,)), dma((2,)), dma((2,)), dma((2,)), dma((2,)),
            dma((5,)), dma((6,)),
            pltpu.SemaphoreType.REGULAR, pltpu.SemaphoreType.REGULAR,
        ],
        cost_estimate=pl.CostEstimate(flops=2 * 10**10, bytes_accessed=10**7, transcendentals=0),
        compiler_params=pltpu.CompilerParams(
            collective_id=0, has_side_effects=True, vmem_limit_bytes=36 << 20
        ),
        name="exchange",
    )(*inputs, count, *params)
    out = pl.pallas_call(
        combine_kernel,
        out_shape=jax.ShapeDtypeStruct((COLS * OUTV, LEV), F32),
        in_specs=[vmem, vmem, vmem, smem],
        out_specs=vmem,
        compiler_params=local(8), name="combine",
    )(returned, kept, route, count)
    return out.reshape(LON, LAT, OUTV, LEV)


def solution(mesh):
    in_specs = (
        P("tile", ("lat", "emu"), None, None),
        P(),
        P("tile", ("lat", "emu")),
        P("tile", ("lat", "emu")),
        P("tile", "lat", "emu", None, None),
        P("tile", "lat", "emu"),
        P(("tile", "lat"), None, None),
        P(("tile", "lat"), None),
        P(("tile", "lat"), None),
        P(("tile", "lat"), None, None, None),
        P(("tile", "lat"), None, None),
        P(("tile", "lat"), None, None),
    )
    out_specs = P("tile", ("lat", "emu"), None, None)
    return jax.shard_map(body, mesh=mesh, in_specs=in_specs, out_specs=out_specs, check_vma=False)
```

```python
import functools

import jax
import jax.numpy as jnp
from jax import lax
from jax.experimental import pallas as pl
from jax.experimental.pallas import tpu as pltpu
from jax.sharding import PartitionSpec as P

MESH = pl.DeviceIdType.MESH
BF16 = jnp.bfloat16
F32 = jnp.float32

NY, NZ, NX = 4, 8, 4
PLANE = NY * NX
PEERS = PLANE * NZ
LON, LAT, VARS, LEV, OUTV = 16, 16, 12, 128, 4
COLS = LON * LAT
ROWS = VARS * LAT
HID = 1024
WORDS = VARS + 1


PIECES = ((0, 48), (48, 80), (80, 128))


def place(step, z_off, me):
    y, z, lat = me
    d_x, d_y = lax.rem(step, NX), lax.div(step, NX)
    tile = lax.rem(y + d_y, NY) * NZ + lax.rem(z + z_off, NZ)
    return tile, lax.rem(lat + d_x, NX)


def source(step, z_off, me):
    y, z, lat = me
    d_x, d_y = lax.rem(step, NX), lax.div(step, NX)
    tile = lax.rem(y + NY - d_y, NY) * NZ + lax.rem(z + NZ - z_off, NZ)
    return tile, lax.rem(lat + NX - d_x, NX)


def slot_row(route_row, count):
    shape = (COLS, COLS)
    first = lax.broadcasted_iota(jnp.int32, shape, 0)
    second = lax.broadcasted_iota(jnp.int32, shape, 1)
    row = jnp.broadcast_to(route_row, shape)
    diagonal = jnp.where(first == second, row, 0.0)
    column = jnp.broadcast_to(jnp.sum(diagonal, axis=1, keepdims=True), shape)
    earlier = (first < second) & (row == column) & (first < count)
    rank = jnp.sum(jnp.where(earlier, 1.0, 0.0), axis=0, keepdims=True)
    position = lax.broadcasted_iota(jnp.int32, (1, COLS), 1)
    return jnp.where(position < count, 2.0 * route_row + rank, -1.0)


def slot_matrix(route_row, count):
    slots = lax.broadcasted_iota(jnp.int32, (COLS, COLS), 0).astype(F32)
    hit = slots == jnp.broadcast_to(slot_row(route_row, count), (COLS, COLS))
    return jnp.where(hit, 1.0, 0.0).astype(BF16)


def as_columns(row, width):
    shape = (LAT, LAT)
    same = lax.broadcasted_iota(jnp.int32, shape, 0) == lax.broadcasted_iota(jnp.int32, shape, 1)
    picked = jnp.where(same, jnp.broadcast_to(row, shape), 0.0)
    return jnp.broadcast_to(jnp.sum(picked, axis=1, keepdims=True), (LAT, width))


def advance(state, halos, diff, wind, land, one_hot, lat, emu, outbound, kept, feats, sides):
    sub = lax.broadcasted_iota(jnp.int32, (LAT, LEV), 0)
    sides[0] = halos[2].astype(F32) * jnp.where((lat == 0) & (emu == 0), 0.0, 1.0).astype(F32)
    sides[1] = halos[3].astype(F32) * jnp.where((lat == NX - 1) & (emu == 1), 0.0, 1.0).astype(F32)

    def one(lon, carry):
        gust = 0.5 * as_columns(wind[pl.ds(lon, 1), :], LEV)
        place_of = pl.ds(pl.multiple_of(lon * LAT, LAT), LAT)
        surface = as_columns(land[pl.ds(lon, 1), :].astype(F32), LEV)
        feats[place_of, VARS * LEV :] = surface.astype(BF16)
        here = lon * ROWS
        east = jnp.minimum(lon + 1, LON - 1) * ROWS
        west = jnp.maximum(lon - 1, 0) * ROWS
        for v in range(VARS):
            inner = slice(v * LAT, (v + 1) * LAT)
            mid = state[pl.ds(pl.multiple_of(here + v * LAT, LAT), LAT), :]
            right = state[pl.ds(pl.multiple_of(east + v * LAT, LAT), LAT), :]
            left = state[pl.ds(pl.multiple_of(west + v * LAT, LAT), LAT), :]
            right = jnp.where(lon == LON - 1, halos[1, inner, :].astype(F32), right)
            left = jnp.where(lon == 0, halos[0, inner, :].astype(F32), left)
            south = jnp.broadcast_to(sides[0, pl.ds(lon * VARS + v, 1), :], (LAT, LEV))
            north = jnp.broadcast_to(sides[1, pl.ds(lon * VARS + v, 1), :], (LAT, LEV))
            up = jnp.where(sub == LAT - 1, north, pltpu.roll(mid, LAT - 1, 0))
            down = jnp.where(sub == 0, south, pltpu.roll(mid, 1, 0))
            spread = right + left + up + down - 4.0 * mid
            moved = mid + diff[v : v + 1, :] * spread - gust * (right - left)
            feats[place_of, v * LEV : (v + 1) * LEV] = moved.astype(BF16)
            if v < OUTV:
                kept[pl.ds(pl.multiple_of((lon * OUTV + v) * LAT, LAT), LAT), :] = moved
        return carry

    lax.fori_loop(0, LON, one, 0)
    for v in range(WORDS):
        rows = jnp.dot(one_hot[...], feats[:, v * LEV : (v + 1) * LEV], preferred_element_type=F32)
        outbound[v] = rows.astype(BF16).reshape(PEERS, 2, LEV)


def position():
    tile, lat, emu = lax.axis_index("tile"), lax.axis_index("lat"), lax.axis_index("emu")
    return (lax.div(tile, NZ), lax.rem(tile, NZ), lat), emu, tile * NX + lat


def z_of(index):
    half = lax.div(index + 1, 2)
    return NZ // 2 + (2 * lax.rem(index, 2) - 1) * half * (-1)


def network(inbound, span, rows, w_in, b_in, land_vec, w_hid, b_hid, w_out):
    taken = jnp.concatenate([inbound[v, span].reshape(rows, LEV) for v in range(VARS)], axis=1)
    flag = inbound[VARS, span].reshape(rows, LEV).astype(F32)
    flag = jnp.concatenate([flag] * (HID // LEV), axis=1)
    hidden = jnp.dot(taken, w_in[...], preferred_element_type=F32)
    hidden = jax.nn.silu(hidden + b_in[...] + flag * land_vec[...]).astype(BF16)
    for layer in range(2):
        inner = jnp.dot(hidden, w_hid[layer], preferred_element_type=F32)
        hidden = jax.nn.silu(inner + b_hid[layer : layer + 1, :]).astype(BF16)
    return jnp.dot(hidden, w_out[...], preferred_element_type=F32).astype(BF16)


def exchange_kernel(
    state_hbm, diff_hbm, wind_hbm, land_hbm, route_hbm, count,
    w_in_hbm, b_in_hbm, land_vec_hbm, w_hid_hbm, b_hid_hbm, w_out_hbm, returned, kept,
    state, diff, wind, land, route, edges, halos, one_hot,
    outbound, inbound, answers, feats, sides, w_in, b_in, land_vec, w_hid, b_hid, w_out,
    edge_send, edge_recv, go_send, go_recv, back_send, back_recv, own_sem, load_sem, weight_sem,
    plane_sem, all_sem,
):
    me, emu, expert = position()
    y, z, lat = me
    tile, tiles = y * NZ + z, NY * NZ
    own_slot = PEERS - PLANE

    east = (lax.rem(tile + 1, tiles), lat, emu)
    west = (lax.rem(tile + tiles - 1, tiles), lat, emu)
    other = (tile, lat, 1 - emu)
    across = (tile, lax.rem(lat + NX - 1 + 2 * emu, NX), 1 - emu)
    x_line = [(tile, lax.rem(lat + d, NX), emu) for d in range(1, NX)]
    y_line = [(lax.rem(y + d, NY) * NZ + z, lat, emu) for d in range(1, NY)]
    z_line = [(y * NZ + lax.rem(z + d, NZ), lat, emu) for d in range(1, NZ)]
    greeted = [east, west, other, across] + x_line + y_line + z_line
    barrier = pltpu.get_barrier_semaphore()
    for device in greeted:
        pl.semaphore_signal(barrier, inc=1, device_id=device, device_id_type=MESH)

    def copies_of(pairs, sems):
        made = [pltpu.make_async_copy(a, b, sems.at[k]) for k, (a, b) in enumerate(pairs)]
        for copy in made:
            copy.start()
        return made

    loads = copies_of(
        ((state_hbm, state), (diff_hbm, diff), (wind_hbm, wind), (land_hbm, land), (route_hbm, route)),
        load_sem,
    )
    weights = copies_of(
        (
            (w_in_hbm, w_in), (b_in_hbm, b_in), (land_vec_hbm, land_vec),
            (w_hid_hbm, w_hid), (b_hid_hbm, b_hid), (w_out_hbm, w_out),
        ),
        weight_sem,
    )
    for copy in loads:
        copy.wait()

    edges[0] = state[pl.ds((LON - 1) * ROWS, ROWS), :].astype(BF16)
    edges[1] = state[pl.ds(0, ROWS), :].astype(BF16)
    edges[2] = state[pl.ds(LAT - 1, LON * VARS, stride=LAT), :].astype(BF16)
    edges[3] = state[pl.ds(0, LON * VARS, stride=LAT), :].astype(BF16)
    pl.semaphore_wait(barrier, len(greeted))
    sent = []
    for k, (edge, device) in enumerate(((0, east), (1, west), (2 + emu, other), (3 - emu, across))):
        copy = pltpu.make_async_remote_copy(
            src_ref=edges.at[edge], dst_ref=halos.at[edge], send_sem=edge_send.at[k],
            recv_sem=edge_recv.at[k], device_id=device, device_id_type=MESH,
        )
        copy.start()
        sent.append(copy)
    for device in y_line:
        pl.semaphore_signal(plane_sem, inc=1, device_id=device, device_id_type=MESH)
    one_hot[...] = slot_matrix(route[...].astype(F32), count[0, 0])
    pl.semaphore_wait(plane_sem, len(y_line))
    for device in z_line:
        pl.semaphore_signal(all_sem, inc=1, device_id=device, device_id_type=MESH)
    for copy in sent:
        copy.wait()
    advance(state, halos, diff, wind, land, one_hot, lat, emu, outbound, kept, feats, sides)
    own = pltpu.make_async_copy(outbound.at[:, expert], inbound.at[:, own_slot], own_sem.at[0])
    own.start()
    pl.semaphore_wait(all_sem, len(z_line))

    def forward(piece, index):
        tile_to, lat_to = place(lax.rem(index, PLANE), z_of(lax.div(index, PLANE)), me)
        return pltpu.make_async_remote_copy(
            src_ref=outbound.at[:, tile_to * NX + lat_to], dst_ref=inbound.at[:, index],
            send_sem=go_send.at[piece], recv_sem=go_recv.at[piece],
            device_id=(tile_to, lat_to, emu), device_id_type=MESH,
        )

    def backward(piece, index):
        tile_to, lat_to = source(lax.rem(index, PLANE), z_of(lax.div(index, PLANE)), me)
        return pltpu.make_async_remote_copy(
            src_ref=answers.at[:, index], dst_ref=returned.at[:, expert],
            send_sem=back_send.at[piece], recv_sem=back_recv.at[piece],
            device_id=(tile_to, lat_to, emu), device_id_type=MESH,
        )

    def start_all(make, piece, first, last):
        def one(index, carry):
            make(piece, index).start()
            return carry

        if first <= own_slot < last:
            lax.fori_loop(first, own_slot, one, 0)
            lax.fori_loop(own_slot + 1, last, one, 0)
        else:
            lax.fori_loop(first, last, one, 0)

    def finish(source_ref, target_ref, send_sem, recv_sem, piece, first, last):
        size = last - first - (1 if first <= own_slot < last else 0)
        pltpu.make_async_remote_copy(
            src_ref=source_ref.at[:, pl.ds(0, size)], dst_ref=target_ref.at[:, pl.ds(0, size)],
            send_sem=send_sem.at[piece], recv_sem=recv_sem.at[piece],
            device_id=(*place(1, 0, me), emu), device_id_type=MESH,
        ).wait()

    for piece, (first, last) in enumerate(PIECES):
        start_all(forward, piece, first, last)
    for piece, (first, last) in enumerate(PIECES):
        finish(outbound, inbound, go_send, go_recv, piece, first, last)
        if piece == 0:
            for copy in weights:
                copy.wait()
        if first <= own_slot < last:
            own.wait()
        span = slice(first, last)
        made = network(
            inbound, span, 2 * (last - first), w_in, b_in, land_vec, w_hid, b_hid, w_out
        )
        for v in range(OUTV):
            part = made[:, v * LEV : (v + 1) * LEV]
            answers[v, span] = part.reshape(last - first, 2, LEV)
        start_all(backward, piece, first, last)
    mine = pltpu.make_async_copy(answers.at[:, own_slot], returned.at[:, expert], own_sem.at[1])
    mine.start()
    for piece, (first, last) in enumerate(PIECES):
        finish(answers, returned, back_send, back_recv, piece, first, last)
    mine.wait()


def combine_kernel(returned, kept, route, count, out):
    one_hot = slot_matrix(route[...].astype(F32), count[0, 0])
    flat = jnp.concatenate([returned[v].reshape(COLS, LEV) for v in range(OUTV)], axis=1)
    tendency = lax.dot_general(
        one_hot, flat, (((0,), (0,)), ((), ())), preferred_element_type=F32
    )
    for lon in range(LON):
        for v in range(OUTV):
            base = kept[pl.ds((lon * OUTV + v) * LAT, LAT), :]
            added = tendency[lon * LAT : (lon + 1) * LAT, v * LEV : (v + 1) * LEV]
            out[pl.ds(lon * LAT * OUTV + v, LAT, stride=OUTV), :] = base + added


def body(state, diff, wind, land, routes, counts, w_in, b_in, land_vec, w_hid, b_hid, w_out):
    flat_state = jnp.transpose(state, (0, 2, 1, 3)).reshape(LON * ROWS, LEV)
    route = routes.reshape(1, COLS)
    count = counts.reshape(1, 1)
    vmem = pl.BlockSpec(memory_space=pltpu.VMEM)
    smem = pl.BlockSpec(memory_space=pltpu.SMEM)
    hbm = pl.BlockSpec(memory_space=pltpu.HBM)
    anywhere = pl.BlockSpec(memory_space=pl.ANY)
    dma = pltpu.SemaphoreType.DMA
    features = jax.ShapeDtypeStruct((WORDS, PEERS, 2, LEV), BF16)
    answer = jax.ShapeDtypeStruct((OUTV, PEERS, 2, LEV), BF16)

    def local(size):
        return pltpu.CompilerParams(vmem_limit_bytes=size << 20)

    def held(*arrays):
        return [pltpu.with_memory_space_constraint(x, pltpu.HBM) for x in arrays]

    inputs = held(flat_state, diff, wind, land, route)
    params = held(w_in[0], b_in, land_vec, w_hid[0], b_hid[0], w_out[0])
    returned, kept = pl.pallas_call(
        exchange_kernel,
        out_shape=(answer, jax.ShapeDtypeStruct((LON * OUTV * LAT, LEV), F32)),
        in_specs=[hbm] * 5 + [smem] + [hbm] * 6,
        out_specs=(anywhere, vmem),
        scratch_shapes=[pltpu.VMEM(x.shape, x.dtype) for x in inputs]
        + [
            pltpu.VMEM((4, ROWS, LEV), BF16),
            pltpu.VMEM((4, ROWS, LEV), BF16),
            pltpu.VMEM((COLS, COLS), BF16),
            pltpu.VMEM(features.shape, BF16),
            pltpu.VMEM(features.shape, BF16),
            pltpu.VMEM(answer.shape, BF16),
            pltpu.VMEM((COLS, WORDS * LEV), BF16),
            pltpu.VMEM((2, ROWS, LEV), F32),
        ]
        + [pltpu.VMEM(x.shape, x.dtype) for x in params]
        + [
            dma((4,)), dma((4,)), dma((3,)), dma((3,)), dma((3,)), dma((3,)), dma((2,)),
            dma((5,)), dma((6,)),
            pltpu.SemaphoreType.REGULAR, pltpu.SemaphoreType.REGULAR,
        ],
        cost_estimate=pl.CostEstimate(flops=2 * 10**10, bytes_accessed=10**7, transcendentals=0),
        compiler_params=pltpu.CompilerParams(
            collective_id=0, has_side_effects=True, vmem_limit_bytes=36 << 20
        ),
        name="exchange",
    )(*inputs, count, *params)
    out = pl.pallas_call(
        combine_kernel,
        out_shape=jax.ShapeDtypeStruct((COLS * OUTV, LEV), F32),
        in_specs=[vmem, vmem, vmem, smem],
        out_specs=vmem,
        compiler_params=local(8), name="combine",
    )(returned, kept, route, count)
    return out.reshape(LON, LAT, OUTV, LEV)


def solution(mesh):
    in_specs = (
        P("tile", ("lat", "emu"), None, None),
        P(),
        P("tile", ("lat", "emu")),
        P("tile", ("lat", "emu")),
        P("tile", "lat", "emu", None, None),
        P("tile", "lat", "emu"),
        P(("tile", "lat"), None, None),
        P(("tile", "lat"), None),
        P(("tile", "lat"), None),
        P(("tile", "lat"), None, None, None),
        P(("tile", "lat"), None, None),
        P(("tile", "lat"), None, None),
    )
    out_specs = P("tile", ("lat", "emu"), None, None)
    return jax.shard_map(body, mesh=mesh, in_specs=in_specs, out_specs=out_specs, check_vma=False)
```
